256 devices in a mesh: dp: 8 (over x, core), expert: 32 (over z, y).
Axes of the slice: x: 4, y: 4, z: 8, core: 2. Of those that a mesh axis runs over, the one named last changes fastest.
Arguments:
- tokens: bfloat16 [5120, 262144], P(None, ('dp', 'expert')), may hold values from -24 to 24, as said below
- router: bfloat16 [5120, 160], P(None, 'expert'), may hold values from -1 to 1, as said below
- device_pick: int32 [3, 262144], P(None, 'dp'), may hold values from 0 to 31, as said below
- expert_pick: int32 [6, 262144], P(None, 'dp'), may hold values from 0 to 159, as said below
Outputs:
- gates: float32 [6, 262144], P(None, 'dp')
- device_max: float32 [32, 262144], P('expert', 'dp')
- balance: float32 [3], replicated
The draws below stay inside these ranges and needn't reach their ends.
Inputs may be any that keep to these rules, and one draw needn't show every extreme that they name: tokens lie within the range; in each column the values are of order one, except in a few columns. router entries are of order 1 / sqrt(5120). `device_pick`: each column names 3 different devices. `expert_pick`: each column names 6 different experts, two on each device of the column's device_pick, in that order; the device of expert e is e // 5.
All inputs are finite; a program needn't handle non-finite values.
Results may differ from the reference program's by a relative error of at most 0.0003.
Values may be sent and summed in bfloat16 or wider, within the bound.
A program may use at most 64 MiB of HBM per device.

```python
import jax
import jax.numpy as jnp
from jax import lax

D = 5120
EXP_DEV = 5
TOP = 6
DEV_TOP = 3
TOK_DEV = 32768
NDEV = 32
E = 160
TOKENS = 262144


def router_base(key):
    values = jax.random.normal(jax.random.fold_in(key, 7), (D, E), jnp.float32)
    return jnp.clip(values, -6.0, 6.0) * D ** (-0.5)


def draw_router(key, part):
    return router_base(key).astype(jnp.bfloat16)


def draw_tokens(key, part):
    inner = jax.random.fold_in(key, 3)
    shared = jax.random.normal(jax.random.fold_in(inner, 1), (D,), jnp.float32) * 0.5
    values = jax.random.normal(jax.random.fold_in(inner, 4), (TOKENS, D), jnp.float32) + shared[None, :]
    return jnp.clip(values, -24.0, 24.0).T.astype(jnp.bfloat16)


def draw_picks(key):
    inner = jax.random.fold_in(key, 11)
    span = max(TOK_DEV // 2, 1)
    blocks = (TOKENS + span - 1) // span
    hot_table = jax.random.randint(jax.random.fold_in(inner, 1), (blocks, 4), 0, NDEV)
    rows = jnp.arange(TOKENS, dtype=jnp.int32)
    hot_rows = hot_table[rows // span]
    slots = jnp.arange(NDEV, dtype=jnp.int32)
    hot = jnp.any(hot_rows[:, :, None] == slots[None, None, :], axis=1).astype(jnp.int32)
    noise = jax.random.randint(jax.random.fold_in(inner, 2), (TOKENS, NDEV), 0, 2 ** 22)
    keyed = (noise + hot * 2 ** 21) * NDEV + slots[None, :]
    _, chosen_dev = lax.top_k(keyed, DEV_TOP)
    chosen_dev = chosen_dev.astype(jnp.int32)
    local_noise = jax.random.randint(jax.random.fold_in(inner, 3), (TOKENS, DEV_TOP, EXP_DEV), 0, 2 ** 20)
    local_keyed = local_noise * EXP_DEV + jnp.arange(EXP_DEV, dtype=jnp.int32)[None, None, :]
    _, local_slot = lax.top_k(local_keyed, 2)
    experts = chosen_dev[:, :, None] * EXP_DEV + local_slot.astype(jnp.int32)
    return (chosen_dev.T, experts.reshape(TOKENS, TOP).T.astype(jnp.int32))


def draw_device_pick(key, part):
    return draw_picks(key)[0]


def draw_expert_pick(key, part):
    return draw_picks(key)[1]


def setup_inputs(seed: int = 0) -> dict:
    keys = jax.random.split(jax.random.key(seed), 5)
    tokens = draw_tokens(jax.random.fold_in(keys[4], 71), 0)
    router = draw_router(jax.random.fold_in(keys[4], 71), 0)
    device_pick = draw_device_pick(jax.random.fold_in(keys[4], 71), 0)
    expert_pick = draw_expert_pick(jax.random.fold_in(keys[4], 71), 0)
    return {"tokens": tokens, "router": router, "device_pick": device_pick, "expert_pick": expert_pick}


def reference(tokens, router, device_pick, expert_pick):
    scores = jnp.dot(router.T, tokens, preferred_element_type=jnp.float32)
    peak = jnp.max(scores, axis=0, keepdims=True)
    raised = jnp.exp(scores - peak)
    probs = raised / jnp.sum(raised, axis=0, keepdims=True)
    gates = jnp.take_along_axis(probs, expert_pick, axis=0)
    device_max = jnp.max(probs.reshape(NDEV, EXP_DEV, TOKENS), axis=1)
    ones_exp = jnp.ones((TOKENS * TOP,), jnp.float32)
    counts = jax.ops.segment_sum(ones_exp, expert_pick.reshape(-1), num_segments=E)
    ones_dev = jnp.ones((TOKENS * DEV_TOP,), jnp.float32)
    sent_counts = jax.ops.segment_sum(ones_dev, device_pick.reshape(-1), num_segments=NDEV)
    freq = counts * (E / (TOP * TOKENS))
    prob = jnp.sum(probs, axis=1) / TOKENS
    dev_freq = jnp.mean(freq.reshape(NDEV, EXP_DEV), axis=1)
    dev_prob = jnp.sum(prob.reshape(NDEV, EXP_DEV), axis=1)
    sent = sent_counts * (NDEV / (DEV_TOP * TOKENS))
    balance = jnp.stack([jnp.sum(freq * prob), jnp.sum(dev_freq * dev_prob), jnp.sum(sent * dev_prob)])
    return gates, device_max, balance
```

```python
import jax
import jax.numpy as jnp
from jax import lax
from jax.experimental import pallas as pl
from jax.experimental.pallas import tpu as pltpu
from jax.sharding import Mesh
from jax.sharding import PartitionSpec as P

AXES = ("x", "core", "z", "y")
NX, NC, NZ, NY = 4, 2, 8, 4
MESH = pl.DeviceIdType.MESH
F32, BF16 = jnp.float32, jnp.bfloat16
TOP, DEV_TOP = 6, 3
EXP_DEV = 5
EXPERTS = EXP_DEV * NZ * NY
FEATURES = 5120
SHARE = 1024
LANE = 128
TILES = SHARE // LANE
CHUNKS = 5
WIDTH = 256
SLICE = CHUNKS * WIDTH
SLABS = NY * EXP_DEV
ROWS = EXP_DEV * NZ
Z_ORDER = (1, 7, 2, 6, 3, 5, 4)
Y_ORDER = (1, 3, 2)


def wrap(value, size):
    return lax.rem(value + size, size)


def kernel(
    tok_hbm, router_ref, dpick_hbm, epick_hbm,
    gates_ref, dmax_ref, bal_ref,
    tok, rl, zb, own, cor, xb, xc, acc, gs, gr, dmb, ps, cs, stz, sty, stx, ep, dpk,
    tok_sem, pick_sem,
    zs, zr, ys, yr, xs, xr, cs_sem, cr_sem, fs, fr,
    gzs, gzr, gys, gyr, ds_, dr, szs, szr, sys_, syr, sxs, sxr,
):
    x, c = lax.axis_index("x"), lax.axis_index("core")
    z, y = lax.axis_index("z"), lax.axis_index("y")
    me = z * NY + y
    parity = lax.rem(x, 2)
    piece = parity * 2 + c
    base_own = piece * SLICE
    base_cor = (parity * 2 + 1 - c) * SLICE
    base_xb = ((1 - parity) * 2 + c) * SLICE
    base_xc = ((1 - parity) * 2 + 1 - c) * SLICE

    pending = []

    def send(src, dst, send_sem, recv_sem, where):
        copy = pltpu.make_async_remote_copy(
            src_ref=src, dst_ref=dst, send_sem=send_sem, recv_sem=recv_sem,
            device_id=where, device_id_type=MESH,
        )
        copy.start()
        pending.append(copy)

    def arrived(dst, send_sem, recv_sem, where):
        pltpu.make_async_remote_copy(
            src_ref=dst, dst_ref=dst, send_sem=send_sem, recv_sem=recv_sem,
            device_id=where, device_id_type=MESH,
        ).wait_recv()

    barrier = pltpu.get_barrier_semaphore()
    for d in range(1, NZ):
        pl.semaphore_signal(barrier, inc=1, device_id={"z": wrap(z + d, NZ)}, device_id_type=MESH)
    for d in range(1, NY):
        pl.semaphore_signal(barrier, inc=1, device_id={"y": wrap(y + d, NY)}, device_id_type=MESH)
    for dx in range(NX):
        for dc in range(NC):
            if dx or dc:
                pl.semaphore_signal(
                    barrier, inc=1,
                    device_id={"x": wrap(x + dx, NX), "core": wrap(c + dc, NC)},
                    device_id_type=MESH,
                )

    tok_copy = pltpu.make_async_copy(tok_hbm, tok, tok_sem)
    tok_copy.start()
    first = pl.multiple_of(me * SHARE, SHARE)
    ep_copy = pltpu.make_async_copy(epick_hbm.at[:, pl.ds(first, SHARE)], ep, pick_sem.at[0])
    dp_copy = pltpu.make_async_copy(dpick_hbm.at[:, pl.ds(first, SHARE)], dpk, pick_sem.at[1])
    ep_copy.start()
    dp_copy.start()

    mine = router_ref[...].astype(F32)
    mine = jnp.concatenate([mine, jnp.zeros((8 - EXP_DEV, FEATURES), F32)], axis=0)
    rl[...] = mine.astype(BF16)

    def columns(i):
        return pl.ds(pl.multiple_of(base_own + i * WIDTH, WIDTH), WIDTH)

    for i in range(CHUNKS):
        zb[i, z] = rl[:, columns(i)]

    pl.semaphore_wait(barrier, NZ + NY + NX * NC - 3)

    for i in range(CHUNKS):
        for d in Z_ORDER:
            send(rl.at[:, columns(i)], zb.at[i, z], zs.at[i, d - 1], zr.at[i, d - 1],
                 {"z": wrap(z + d, NZ)})

    ep_copy.wait()
    dp_copy.wait()
    sub = lax.broadcasted_iota(jnp.int32, (8, LANE), 0)
    lane = lax.broadcasted_iota(jnp.int32, (8, LANE), 1)
    cs[...] = jnp.zeros_like(cs)
    ps[...] = jnp.zeros_like(ps)

    def count(lt, carry):
        off = pl.ds(pl.multiple_of(lt * LANE, LANE), LANE)
        diffs = [ep[pl.ds(k, 1), off] - 20 * sub for k in range(TOP)]
        for s in range(SLABS):
            hit = diffs[0] == s
            for k in range(1, TOP):
                hit = hit | (diffs[k] == s)
            cs[s] += jnp.where(hit, 1.0, 0.0)
        diffs = [dpk[pl.ds(k, 1), off] - NY * sub for k in range(DEV_TOP)]
        for s in range(NY):
            hit = (diffs[0] == s) | (diffs[1] == s) | (diffs[2] == s)
            cs[SLABS + s] += jnp.where(hit, 1.0, 0.0)
        return carry

    lax.fori_loop(0, TILES, count, 0)

    def packed(ref, rows, offset, into):
        sums = [jnp.sum(ref[s], axis=1, keepdims=True) for s in range(rows)]
        for s in range(rows):
            into = into + jnp.where(lane == offset + s, sums[s], 0.0)
        for group in range(NY if rows >= SLABS else 0):
            total = sums[group * EXP_DEV]
            for j in range(1, EXP_DEV):
                total = total + sums[group * EXP_DEV + j]
            into = into + jnp.where(lane == offset + SLABS + group, total, 0.0)
            if offset == 0:
                into = into + jnp.where(lane == SLABS + NY + group, total, 0.0)
        if rows > SLABS:
            pass
        return into

    stats = packed(cs, SLABS, 64, jnp.zeros((8, LANE), F32))
    for group in range(NY):
        stats = stats + jnp.where(
            lane == 64 + SLABS + NY + group,
            jnp.sum(cs[SLABS + group], axis=1, keepdims=True), 0.0)

    row = lax.broadcasted_iota(jnp.int32, (ROWS, 8 * NZ), 0)
    col = lax.broadcasted_iota(jnp.int32, (ROWS, 8 * NZ), 1)
    order = (col == (row % 8) * 8 + row // 8).astype(BF16)

    for i in range(CHUNKS):
        for d in Z_ORDER:
            arrived(zb.at[i, wrap(z - d, NZ)], zs.at[i, d - 1], zr.at[i, d - 1], {"z": wrap(z + d, NZ)})
        block = jnp.dot(order, zb[i].reshape(8 * NZ, WIDTH), preferred_element_type=F32)
        own[i, y] = block.astype(BF16)
        for d in Y_ORDER:
            send(own.at[i, y], own.at[i, y], ys.at[i, d - 1], yr.at[i, d - 1], {"y": wrap(y + d, NY)})

    tok_copy.wait()

    def multiply(ref, i, base, fresh=False):
        left = ref[i].reshape(NY * ROWS, WIDTH)
        right = tok[pl.ds(pl.multiple_of(base + i * WIDTH, WIDTH), WIDTH), :]
        out = jnp.dot(left, right, preferred_element_type=F32)
        if fresh:
            acc[...] = out
        else:
            acc[...] += out

    right_x, left_x = {"x": wrap(x + 1, NX)}, {"x": wrap(x - 1, NX)}
    other = {"core": 1 - c}
    HALF = WIDTH // 2
    for i in range(CHUNKS):
        for d in Y_ORDER:
            arrived(own.at[i, wrap(y - d, NY)], ys.at[i, d - 1], yr.at[i, d - 1], {"y": wrap(y + d, NY)})
        if i < CHUNKS - 1:
            send(own.at[i], xb.at[i], xs.at[i], xr.at[i], right_x if i % 2 == 0 else left_x)
        else:
            for h, where in enumerate((right_x, left_x)):
                part = pl.ds(h * HALF, HALF)
                send(own.at[i, :, :, part], xb.at[i, :, :, part], xs.at[i + h], xr.at[i + h], where)
        send(own.at[i], cor.at[i], cs_sem.at[i], cr_sem.at[i], other)
        multiply(own, i, base_own, fresh=i == 0)
    for i in range(CHUNKS):
        arrived(cor.at[i], cs_sem.at[i], cr_sem.at[i], other)
        multiply(cor, i, base_cor)
    for i in range(CHUNKS):
        if i < CHUNKS - 1:
            arrived(xb.at[i], xs.at[i], xr.at[i], right_x)
        else:
            for h in range(2):
                part = pl.ds(h * HALF, HALF)
                arrived(xb.at[i, :, :, part], xs.at[i + h], xr.at[i + h], right_x)
        send(xb.at[i], xc.at[i], fs.at[i], fr.at[i], other)
        multiply(xb, i, base_xb)
    for i in range(CHUNKS):
        arrived(xc.at[i], fs.at[i], fr.at[i], other)
        multiply(xc, i, base_xc)

    def tree(op, values):
        while len(values) > 1:
            values = [op(*values[n:n + 2]) if n + 1 < len(values) else values[n]
                      for n in range(0, len(values), 2)]
        return values[0]

    def column(lt, carry):
        off = pl.ds(pl.multiple_of(lt * LANE, LANE), LANE)
        score = [acc[pl.ds(s * 8, 8), off] for s in range(SLABS)]
        peak = jnp.max(tree(jnp.maximum, score), axis=0, keepdims=True)
        raised = [jnp.exp(v - peak) for v in score]
        total = jnp.sum(tree(jnp.add, raised), axis=0, keepdims=True)
        inv = 1.0 / total
        prob = [v * inv for v in raised]
        for group in range(NY):
            top = tree(jnp.maximum, prob[group * EXP_DEV:(group + 1) * EXP_DEV])
            dmb[pl.ds(group * TILES + lt, NZ, stride=NY * TILES), :] = top
        for k in range(TOP):
            diff = ep[pl.ds(k, 1), off] - 20 * sub
            chosen = jnp.zeros((8, LANE), F32)
            for s in range(SLABS):
                chosen = jnp.where(diff == s, prob[s], chosen)
            gs[pl.ds(k * TILES + lt, 1), :] = jnp.sum(chosen, axis=0, keepdims=True)
        for s in range(SLABS):
            ps[s] += prob[s]
        return carry

    lax.fori_loop(0, TILES, column, 0)
    gr[z, y] = gs[...]

    for d in Z_ORDER:
        send(gs, gr.at[z, y], gzs.at[d - 1], gzr.at[d - 1], {"z": wrap(z + d, NZ)})
    for d in Y_ORDER:
        send(gs, gr.at[z, y], gys.at[0, d - 1], gyr.at[0, d - 1], {"y": wrap(y + d, NY)})

    stats = packed(ps, SLABS, 0, stats)
    stz[z] = stats
    for d in Z_ORDER:
        send(stz.at[z], stz.at[z], szs.at[d - 1], szr.at[d - 1], {"z": wrap(z + d, NZ)})

    for dz in range(NZ):
        for dy in range(NY):
            n = dz * NY + dy
            if n == 0:
                continue
            zt, yt = wrap(z + dz, NZ), wrap(y + dy, NY)
            send(dmb.at[pl.ds(pl.multiple_of((zt * NY + yt) * TILES, TILES), TILES), :],
                 dmax_ref.at[pl.ds(pl.multiple_of(me * TILES, TILES), TILES), :],
                 ds_.at[n], dr.at[n], {"z": zt, "y": yt})
    here = pl.ds(pl.multiple_of(me * TILES, TILES), TILES)
    dmax_ref[here, :] = dmb[here, :]

    def forward(d):
        zt = wrap(z - d, NZ)
        arrived(gr.at[zt, y], gzs.at[d - 1], gzr.at[d - 1], {"z": wrap(z + d, NZ)})
        for e in Y_ORDER:
            send(gr.at[zt, y], gr.at[zt, y], gys.at[d, e - 1], gyr.at[d, e - 1], {"y": wrap(y + e, NY)})

    def write(zt, yt):
        block = pl.multiple_of((zt * NY + yt) * SHARE, SHARE)

        def put(lt, carry):
            gates_ref[:, pl.ds(pl.multiple_of(block + lt * LANE, LANE), LANE)] = (
                gr[zt, yt, pl.ds(lt, TOP, stride=TILES), :])
            return carry

        lax.fori_loop(0, TILES, put, 0)

    for d in Z_ORDER:
        forward(d)

    total = stats
    for d in range(1, NZ):
        arrived(stz.at[wrap(z - d, NZ)], szs.at[d - 1], szr.at[d - 1], {"z": wrap(z + d, NZ)})
    total = tree(jnp.add, [stz[n] for n in range(NZ)])
    sty[y] = total
    for d in Y_ORDER:
        send(sty.at[y], sty.at[y], sys_.at[d - 1], syr.at[d - 1], {"y": wrap(y + d, NY)})
    for d in (0,) + Z_ORDER:
        write(wrap(z - d, NZ), y)
    for d in Y_ORDER:
        arrived(sty.at[wrap(y - d, NY)], sys_.at[d - 1], syr.at[d - 1], {"y": wrap(y + d, NY)})
    total = tree(jnp.add, [sty[n] for n in range(NY)])
    slot = x * NC + c
    stx[slot] = total
    for n in range(1, NX * NC):
        dx, dc = n // NC, n % NC
        send(stx.at[slot], stx.at[slot], sxs.at[n], sxr.at[n],
             {"x": wrap(x + dx, NX), "core": wrap(c + dc, NC)})
    for d in (0,) + Z_ORDER:
        for e in Y_ORDER:
            zt, yt = wrap(z - d, NZ), wrap(y - e, NY)
            arrived(gr.at[zt, yt], gys.at[d, e - 1], gyr.at[d, e - 1], {"y": wrap(y + e, NY)})
            write(zt, yt)
    for n in range(1, NX * NC):
        dx, dc = n // NC, n % NC
        xt, ct = wrap(x - dx, NX), wrap(c - dc, NC)
        arrived(stx.at[xt * NC + ct], sxs.at[n], sxr.at[n], {"x": wrap(x + dx, NX), "core": ct})
    total = tree(jnp.add, [stx[n] for n in range(NX * NC)])
    tokens = SHARE * NZ * NY * NX * NC
    product = total * pltpu.roll(total, 64, 1)
    for n, (low, high, scale) in enumerate((
        (0, SLABS, EXPERTS / (TOP * tokens) / tokens),
        (SLABS, SLABS + NY, EXPERTS / EXP_DEV / (TOP * tokens) / tokens),
        (SLABS + NY, SLABS + 2 * NY, NZ * NY / (DEV_TOP * tokens) / tokens),
    )):
        inside = (lane >= low) & (lane < high)
        bal_ref[n] = jnp.sum(jnp.where(inside, product, 0.0)) * scale

    for dz in range(NZ):
        for dy in range(NY):
            n = dz * NY + dy
            if n == 0:
                continue
            zt, yt = wrap(z - dz, NZ), wrap(y - dy, NY)
            spot = pl.ds(pl.multiple_of((zt * NY + yt) * TILES, TILES), TILES)
            arrived(dmax_ref.at[spot, :], ds_.at[n], dr.at[n], {"z": wrap(z + dz, NZ), "y": wrap(y + dy, NY)})
    for copy in pending:
        copy.wait_send()


def local(tokens, router, device_pick, expert_pick):
    dma = pltpu.SemaphoreType.DMA
    vmem, hbm = pl.BlockSpec(memory_space=pltpu.VMEM), pl.BlockSpec(memory_space=pl.ANY)
    group = SHARE * NZ * NY
    gates, dmax, balance = pl.pallas_call(
        kernel,
        out_shape=(
            jax.ShapeDtypeStruct((TOP, group), F32),
            jax.ShapeDtypeStruct((group // LANE, LANE), F32),
            jax.ShapeDtypeStruct((3,), F32),
        ),
        in_specs=[hbm, vmem, hbm, hbm],
        out_specs=(vmem, vmem, pl.BlockSpec(memory_space=pltpu.SMEM)),
        scratch_shapes=[
            pltpu.VMEM((FEATURES, SHARE), BF16),
            pltpu.VMEM((8, FEATURES), BF16),
            pltpu.VMEM((CHUNKS, NZ, 8, WIDTH), BF16),
            *[pltpu.VMEM((CHUNKS, NY, ROWS, WIDTH), BF16) for _ in range(4)],
            pltpu.VMEM((EXPERTS, SHARE), F32),
            pltpu.VMEM((TOP * TILES, LANE), F32),
            pltpu.VMEM((NZ, NY, TOP * TILES, LANE), F32),
            pltpu.VMEM((NZ * NY * TILES, LANE), F32),
            pltpu.VMEM((SLABS, 8, LANE), F32),
            pltpu.VMEM((SLABS + NY, 8, LANE), F32),
            pltpu.VMEM((NZ, 8, LANE), F32),
            pltpu.VMEM((NY, 8, LANE), F32),
            pltpu.VMEM((NX * NC, 8, LANE), F32),
            pltpu.VMEM((TOP, SHARE), jnp.int32),
            pltpu.VMEM((DEV_TOP, SHARE), jnp.int32),
            dma, dma((2,)),
            dma((CHUNKS, NZ - 1)), dma((CHUNKS, NZ - 1)),
            dma((CHUNKS, NY - 1)), dma((CHUNKS, NY - 1)),
            dma((CHUNKS + 1,)), dma((CHUNKS + 1,)),
            dma((CHUNKS,)), dma((CHUNKS,)),
            dma((CHUNKS,)), dma((CHUNKS,)),
            dma((NZ - 1,)), dma((NZ - 1,)),
            dma((NZ, NY - 1)), dma((NZ, NY - 1)),
            dma((NZ * NY,)), dma((NZ * NY,)),
            dma((NZ - 1,)), dma((NZ - 1,)),
            dma((NY - 1,)), dma((NY - 1,)),
            dma((NX * NC,)), dma((NX * NC,)),
        ],
        compiler_params=pltpu.CompilerParams(
            collective_id=0, has_side_effects=True, vmem_limit_bytes=40 * 1024 * 1024,
        ),
    )(tokens, router.T, device_pick, expert_pick)
    return gates, dmax.reshape(1, group), balance


def solution(mesh):
    torus = Mesh(mesh.devices.reshape(NX, NC, NZ, NY), AXES)
    return jax.shard_map(
        local,
        mesh=torus,
        in_specs=(
            P(None, AXES), P(None, ("z", "y")), P(None, ("x", "core")), P(None, ("x", "core")),
        ),
        out_specs=(P(None, ("x", "core")), P(("z", "y"), ("x", "core")), P()),
        check_vma=False,
    )
```

```python
import jax
import jax.numpy as jnp
from jax import lax
from jax.experimental import pallas as pl
from jax.experimental.pallas import tpu as pltpu
from jax.sharding import Mesh
from jax.sharding import PartitionSpec as P

AXES = ("x", "core", "z", "y")
NX, NC, NZ, NY = 4, 2, 8, 4
PEERS, GROUPS = NZ * NY, NX * NC
MESH = pl.DeviceIdType.MESH
F32, BF16 = jnp.float32, jnp.bfloat16
TOP, DEV_TOP = 6, 3
EXP_DEV = 5
EXPERTS = EXP_DEV * NZ * NY
FEATURES = 5120
SHARE = 1024
LANE = 128
TILES = SHARE // LANE
CHUNKS = 5
WIDTH = 256
SLICE = CHUNKS * WIDTH
SLABS = NY * EXP_DEV
ROWS = EXP_DEV * NZ
FINE, COARSE = 2048.0, 455.0
KNEE = 16.0 * (FINE - COARSE)
GRANT = 56080000
Z_ORDER = (1, 7, 2, 6, 3, 5, 4)
Y_ORDER = (1, 3, 2)


def wrap(value, size):
    return lax.rem(value + size, size)


def kernel(
    tok_hbm, router_hbm, dpick_hbm, epick_hbm,
    g0, g1, g2, g3, g4, g5, g6, g7, dmr, bal_ref,
    tok, rt, rl, zb, own, cor, xb, xc, acc, gf, gs, dmf, dms, ps, cs, stz, sty, stx, wt, sv, sx, ep, dpk, wide,
    tok_sem, pick_sem, zs, zr, ys, yr, xs, xr, crs, crr, fs, fr, gzs, gzr, gys, gyr, one_s, one_r,
):
    gates = (g0, g1, g2, g3, g4, g5, g6, g7)
    x, c = lax.axis_index("x"), lax.axis_index("core")
    z, y = lax.axis_index("z"), lax.axis_index("y")
    me = z * NY + y
    parity = lax.rem(x, 2)
    piece = parity * 2 + c
    base_own = piece * SLICE
    base_cor = (parity * 2 + 1 - c) * SLICE
    base_xb = ((1 - parity) * 2 + c) * SLICE
    base_xc = ((1 - parity) * 2 + 1 - c) * SLICE

    first = pl.multiple_of(me * SHARE, SHARE)
    rt_copy = pltpu.make_async_copy(router_hbm, rt, pick_sem.at[2])
    ep_copy = pltpu.make_async_copy(epick_hbm.at[:, pl.ds(first, SHARE)], ep, pick_sem.at[0])
    dp_copy = pltpu.make_async_copy(dpick_hbm.at[:, pl.ds(first, SHARE)], dpk, pick_sem.at[1])
    tok_copy = pltpu.make_async_copy(tok_hbm, tok, tok_sem)
    rt_copy.start()
    ep_copy.start()
    dp_copy.start()
    tok_copy.start()

    def send(src, dst, send_sem, recv_sem, where):
        pltpu.make_async_remote_copy(
            src_ref=src, dst_ref=dst, send_sem=send_sem, recv_sem=recv_sem,
            device_id=where, device_id_type=MESH,
        ).start()

    def took(ref, sem):
        pltpu.make_async_copy(ref, ref, sem).wait()

    def to_z(d):
        return {"z": wrap(z + d, NZ)}

    def to_y(d):
        return {"y": wrap(y + d, NY)}

    def to_zy(n):
        return {"z": wrap(z + n // NY, NZ), "y": wrap(y + n % NY, NY)}

    def to_xc(n):
        return {"x": wrap(x + n // NC, NX), "core": wrap(c + n % NC, NC)}

    def tree(op, values):
        while len(values) > 1:
            values = [op(*values[n:n + 2]) if n + 1 < len(values) else values[n]
                      for n in range(0, len(values), 2)]
        return values[0]

    barrier = pltpu.get_barrier_semaphore()
    for where in (*map(to_z, Z_ORDER), *map(to_y, Y_ORDER), *map(to_xc, range(1, GROUPS))):
        pl.semaphore_signal(barrier, inc=1, device_id=where, device_id_type=MESH)

    rt_copy.wait()
    mine = rt[...].astype(F32)
    mine = jnp.concatenate([mine, jnp.zeros((8 - EXP_DEV, FEATURES), F32)], axis=0)
    rl[...] = mine.astype(BF16)

    def columns(i):
        return pl.ds(pl.multiple_of(base_own + i * WIDTH, WIDTH), WIDTH)

    for i in range(CHUNKS):
        zb[i, z] = rl[:, columns(i)]

    pl.semaphore_wait(barrier, NZ + NY + GROUPS - 3)

    for i in range(CHUNKS):
        for d in Z_ORDER:
            send(rl.at[:, columns(i)], zb.at[i, z], zs.at[i], zr.at[i], to_z(d))

    ep_copy.wait()
    dp_copy.wait()
    sub = lax.broadcasted_iota(jnp.int32, (8, LANE), 0)
    lane = lax.broadcasted_iota(jnp.int32, (8, LANE), 1)
    cs[...] = jnp.zeros_like(cs)
    ps[...] = jnp.zeros_like(ps)

    def count(lt, carry):
        off = pl.ds(pl.multiple_of(lt * LANE, LANE), LANE)
        diffs = [ep[pl.ds(k, 1), off] - 20 * sub for k in range(TOP)]
        for s in range(SLABS):
            hit = diffs[0] == s
            for k in range(1, TOP):
                hit = hit | (diffs[k] == s)
            cs[s] += jnp.where(hit, 1.0, 0.0)
        diffs = [dpk[pl.ds(k, 1), off] - NY * sub for k in range(DEV_TOP)]
        for s in range(NY):
            hit = (diffs[0] == s) | (diffs[1] == s) | (diffs[2] == s)
            cs[SLABS + s] += jnp.where(hit, 1.0, 0.0)
        return carry

    lax.fori_loop(0, TILES, count, 0)

    def packed(ref, base):
        sums = [jnp.sum(ref[s], axis=1, keepdims=True) for s in range(SLABS)]
        into = jnp.zeros((8, LANE), F32)
        for s in range(SLABS):
            into = jnp.where(lane == base + s, sums[s], into)
        groups = [tree(jnp.add, sums[g * EXP_DEV:(g + 1) * EXP_DEV]) for g in range(NY)]
        for g in range(NY):
            into = jnp.where(lane == base + SLABS + g, groups[g], into)
        return into, groups

    stats, _ = packed(cs, 0)
    for g in range(NY):
        there = jnp.sum(cs[SLABS + g], axis=1, keepdims=True)
        stats = jnp.where(lane == SLABS + NY + g, there, stats)
    stz[z] = stats
    for d in Z_ORDER:
        send(stz.at[z], stz.at[z], one_s.at[0], one_r.at[0], to_z(d))

    row = lax.broadcasted_iota(jnp.int32, (ROWS, 8 * NZ), 0)
    col = lax.broadcasted_iota(jnp.int32, (ROWS, 8 * NZ), 1)
    order = (col == (row % 8) * 8 + row // 8).astype(BF16)

    for i in range(CHUNKS):
        took(zb.at[i, pl.ds(0, NZ - 1)], zr.at[i])
        block = jnp.dot(order, zb[i].reshape(8 * NZ, WIDTH), preferred_element_type=F32)
        own[i, y] = block.astype(BF16)
        for d in Y_ORDER:
            send(own.at[i, y], own.at[i, y], ys.at[i], yr.at[i], to_y(d))

    took(stz.at[pl.ds(0, NZ - 1)], one_r.at[0])
    sty[y] = tree(jnp.add, [stz[n] for n in range(NZ)])
    for d in Y_ORDER:
        send(sty.at[y], sty.at[y], one_s.at[1], one_r.at[1], to_y(d))

    tok_copy.wait()

    def multiply(ref, i, base, fresh=False):
        left = ref[i].reshape(NY * ROWS, WIDTH)
        right = tok[pl.ds(pl.multiple_of(base + i * WIDTH, WIDTH), WIDTH), :]
        out = jnp.dot(left, right, preferred_element_type=F32)
        if fresh:
            acc[...] = out
        else:
            acc[...] += out

    right_x, left_x = {"x": wrap(x + 1, NX)}, {"x": wrap(x - 1, NX)}
    other = {"core": 1 - c}
    HALF = WIDTH // 2
    for i in range(CHUNKS):
        took(own.at[i, pl.ds(0, NY - 1)], yr.at[i])
        if i < CHUNKS - 1:
            send(own.at[i], xb.at[i], xs, xr.at[i], right_x if i % 2 == 0 else left_x)
        else:
            for h, where in enumerate((right_x, left_x)):
                part = pl.ds(h * HALF, HALF)
                send(own.at[i, :, :, part], xb.at[i, :, :, part], xs, xr.at[i], where)
        send(own.at[i], cor.at[i], crs, crr.at[i], other)
        multiply(own, i, base_own, fresh=i == 0)
    took(sty.at[pl.ds(0, NY - 1)], one_r.at[1])
    slot = x * NC + c
    stx[slot] = tree(jnp.add, [sty[n] for n in range(NY)])
    for n in range(1, GROUPS):
        send(stx.at[slot], stx.at[slot], one_s.at[2], one_r.at[2], to_xc(n))
    for i in range(CHUNKS):
        took(cor.at[i], crr.at[i])
        multiply(cor, i, base_cor)
    for i in range(CHUNKS):
        took(xb.at[i], xr.at[i])
        send(xb.at[i], xc.at[i], fs, fr.at[i], other)
        multiply(xb, i, base_xb)
    took(stx.at[pl.ds(0, GROUPS - 1)], one_r.at[2])
    wt[...] = tree(jnp.add, [stx[n] for n in range(GROUPS)])
    for i in range(CHUNKS):
        took(xc.at[i], fr.at[i])
        multiply(xc, i, base_xc)

    def coded(log_prob):
        fall = -log_prob
        code = jnp.minimum(fall * FINE, fall * COARSE + KNEE)
        return jnp.clip(jnp.round(code), 0.0, 65535.0) - 32768.0

    def column(lt, carry):
        off = pl.ds(pl.multiple_of(lt * LANE, LANE), LANE)
        score = [acc[pl.ds(s * 8, 8), off] for s in range(SLABS)]
        peak = jnp.max(tree(jnp.maximum, score), axis=0, keepdims=True)
        raised = [jnp.exp(v - peak) for v in score]
        total = jnp.sum(tree(jnp.add, raised), axis=0, keepdims=True)
        inv = 1.0 / total
        shift = peak + jnp.log(total)
        for g in range(NY):
            top = tree(jnp.maximum, score[g * EXP_DEV:(g + 1) * EXP_DEV])
            dmf[pl.ds(g * TILES + lt, NZ, stride=NY * TILES), :] = coded(top - shift)
        for k in range(TOP):
            diff = ep[pl.ds(k, 1), off] - 20 * sub
            chosen = jnp.zeros((8, LANE), F32)
            for s in range(SLABS):
                chosen = jnp.where(diff == s, score[s], chosen)
            gf[pl.ds(k * TILES + lt, 1), :] = coded(jnp.sum(chosen, axis=0, keepdims=True) - shift)
        for s in range(SLABS):
            ps[s] += raised[s] * inv
        return carry

    lax.fori_loop(0, TILES, column, 0)

    sums, groups = packed(ps, 0)
    for g in range(NY):
        sums = jnp.where(lane == SLABS + NY + g, groups[g], sums)
    sv[me] = jnp.sum(sums * wt[...], axis=0, keepdims=True)
    for n in range(1, PEERS):
        send(sv.at[me], sv.at[me], one_s.at[3], one_r.at[3], to_zy(n))

    gs[...] = gf[...].astype(jnp.int32).astype(jnp.int16)
    for d in Z_ORDER:
        send(gs, gates[d].at[y], gzs, gzr.at[d - 1], to_z(d))
    for d in Y_ORDER:
        send(gs, g0.at[y], gys.at[0], gyr.at[0], to_y(d))
    g0[y] = gs[...]
    for n in range(PEERS):
        dms[n] = dmf[n * TILES:(n + 1) * TILES, :].astype(jnp.int32).astype(jnp.int16)
    dmr[me] = dms[me]

    for turn, d in enumerate(Z_ORDER):
        if turn == 2:
            for n in range(1, PEERS):
                there = wrap(z + n // NY, NZ) * NY + wrap(y + n % NY, NY)
                send(dms.at[there], dmr.at[me], one_s.at[4], one_r.at[4], to_zy(n))
        took(gs, gzr.at[d - 1])
        for e in Y_ORDER:
            send(gates[d].at[y], gates[d].at[y], gys.at[d], gyr.at[d], to_y(e))

    took(sv.at[pl.ds(0, PEERS - 1)], one_r.at[3])
    sx[slot] = tree(jnp.add, [sv[n] for n in range(PEERS)])
    for n in range(1, GROUPS):
        send(sx.at[slot], sx.at[slot], one_s.at[5], one_r.at[5], to_xc(n))

    for d in (0,) + Z_ORDER:
        took(gates[d].at[pl.ds(0, NY - 1)], gyr.at[d])

    took(dmr.at[pl.ds(0, PEERS - 1)], one_r.at[4])

    took(sx.at[pl.ds(0, GROUPS - 1)], one_r.at[5])
    bal_ref[...] = jnp.broadcast_to(tree(jnp.add, [sx[n] for n in range(GROUPS)]), (8, LANE))

    for i in range(CHUNKS):
        took(zb.at[i, pl.ds(0, NZ - 1)], zs.at[i])
        took(own.at[i, pl.ds(0, NY - 1)], ys.at[i])
    took(own, xs)
    took(own, crs)
    took(own, fs)
    took(g0.at[pl.ds(0, NY - 1)], gys.at[0])
    for d in Z_ORDER:
        took(g0.at[pl.ds(0, NY - 1)], gys.at[d])
    took(wide.at[pl.ds(0, (NZ - 1) * TOP)], gzs)
    for n, ref in enumerate((
        stz.at[pl.ds(0, NZ - 1)], sty.at[pl.ds(0, NY - 1)], stx.at[pl.ds(0, GROUPS - 1)],
        sv.at[pl.ds(0, PEERS - 1)], dmr.at[pl.ds(0, PEERS - 1)], sx.at[pl.ds(0, GROUPS - 1)],
    )):
        took(ref, one_s.at[n])


def decode(
    g0, g1, g2, g3, g4, g5, g6, g7, dmr, bal_ref,
    gates_hbm, dmax_hbm, balance_ref,
    gf, gates, dmax, out_sem,
):
    z = lax.axis_index("z")

    def plain(codes):
        code = codes.astype(jnp.int32).astype(F32) + 32768.0
        return jnp.exp(jnp.minimum(code * (-1.0 / FINE), (KNEE - code) * (1.0 / COARSE)))

    dmax_out = pltpu.make_async_copy(dmax, dmax_hbm, out_sem.at[NZ])
    for n in range(PEERS):
        dmax[n * TILES:(n + 1) * TILES, :] = plain(dmr[n])
    dmax_out.start()
    outs = [dmax_out]
    for d, ref in enumerate((g0, g1, g2, g3, g4, g5, g6, g7)):
        for n in range(NY):
            gf[n] = plain(ref[n])
            for lt in range(TILES):
                start = n * SHARE + lt * LANE
                gates[d, :, start:start + LANE] = gf[n, pl.ds(lt, TOP, stride=TILES), :]
        block = pl.ds(pl.multiple_of(wrap(z - d, NZ) * NY * SHARE, NY * SHARE), NY * SHARE)
        out = pltpu.make_async_copy(gates.at[d], gates_hbm.at[:, block], out_sem.at[d])
        out.start()
        outs.append(out)
    tokens = SHARE * PEERS * GROUPS
    lane = lax.broadcasted_iota(jnp.int32, (1, LANE), 1)
    for n, (low, high, scale) in enumerate((
        (0, SLABS, EXPERTS / (TOP * tokens) / tokens),
        (SLABS, SLABS + NY, EXPERTS / EXP_DEV / (TOP * tokens) / tokens),
        (SLABS + NY, SLABS + 2 * NY, PEERS / (DEV_TOP * tokens) / tokens),
    )):
        inside = (lane >= low) & (lane < high)
        balance_ref[n] = jnp.sum(jnp.where(inside, bal_ref[:1, :], 0.0)) * scale
    for out in outs:
        out.wait()


def local(tokens, router, device_pick, expert_pick):
    dma = pltpu.SemaphoreType.DMA
    I16, I32 = jnp.int16, jnp.int32
    vmem, hbm = pl.BlockSpec(memory_space=pltpu.VMEM), pl.BlockSpec(memory_space=pltpu.HBM)
    group = SHARE * PEERS
    received = pl.pallas_call(
        kernel,
        out_shape=(
            *[jax.ShapeDtypeStruct((NY, TOP * TILES, LANE), I16) for _ in range(NZ)],
            jax.ShapeDtypeStruct((PEERS, TILES, LANE), I16),
            jax.ShapeDtypeStruct((8, LANE), F32),
        ),
        in_specs=[hbm] * 4,
        out_specs=(vmem,) * (NZ + 2),
        scratch_shapes=[
            pltpu.VMEM((FEATURES, SHARE), BF16),
            pltpu.VMEM((EXP_DEV, FEATURES), BF16),
            pltpu.VMEM((8, FEATURES), BF16),
            pltpu.VMEM((CHUNKS, NZ, 8, WIDTH), BF16),
            *[pltpu.VMEM((CHUNKS, NY, ROWS, WIDTH), BF16) for _ in range(4)],
            pltpu.VMEM((EXPERTS, SHARE), F32),
            pltpu.VMEM((TOP * TILES, LANE), F32),
            pltpu.VMEM((TOP * TILES, LANE), I16),
            pltpu.VMEM((PEERS * TILES, LANE), F32),
            pltpu.VMEM((PEERS, TILES, LANE), I16),
            pltpu.VMEM((SLABS, 8, LANE), F32),
            pltpu.VMEM((SLABS + NY, 8, LANE), F32),
            pltpu.VMEM((NZ, 8, LANE), F32),
            pltpu.VMEM((NY, 8, LANE), F32),
            pltpu.VMEM((GROUPS, 8, LANE), F32),
            pltpu.VMEM((8, LANE), F32),
            pltpu.VMEM((PEERS, 1, LANE), F32),
            pltpu.VMEM((GROUPS, 1, LANE), F32),
            pltpu.VMEM((TOP, SHARE), I32),
            pltpu.VMEM((DEV_TOP, SHARE), I32),
            pltpu.VMEM(((NZ - 1) * TOP, TILES, LANE), I16),
            dma, dma((3,)),
            dma((CHUNKS,)), dma((CHUNKS,)),
            dma((CHUNKS,)), dma((CHUNKS,)),
            dma, dma((CHUNKS,)),
            dma, dma((CHUNKS,)),
            dma, dma((CHUNKS,)),
            dma, dma((NZ - 1,)),
            dma((NZ,)), dma((NZ,)),
            dma((6,)), dma((6,)),
        ],
        compiler_params=pltpu.CompilerParams(
            collective_id=0, has_side_effects=True, vmem_limit_bytes=GRANT,
        ),
    )(tokens, router.T, device_pick, expert_pick)
    gates, dmax, balance = pl.pallas_call(
        decode,
        out_shape=(
            jax.ShapeDtypeStruct((TOP, group), F32),
            jax.ShapeDtypeStruct((group // LANE, LANE), F32),
            jax.ShapeDtypeStruct((3,), F32),
        ),
        in_specs=[vmem] * (NZ + 2),
        out_specs=(hbm, hbm, pl.BlockSpec(memory_space=pltpu.SMEM)),
        scratch_shapes=[
            pltpu.VMEM((NY, TOP * TILES, LANE), F32),
            pltpu.VMEM((NZ, TOP, NY * SHARE), F32),
            pltpu.VMEM((PEERS * TILES, LANE), F32),
            dma((NZ + 1,)),
        ],
        compiler_params=pltpu.CompilerParams(vmem_limit_bytes=16 * 1024 * 1024),
    )(*received)
    return gates, dmax.reshape(1, group), balance


def solution(mesh):
    torus = Mesh(mesh.devices.reshape(NX, NC, NZ, NY), AXES)
    return jax.shard_map(
        local,
        mesh=torus,
        in_specs=(
            P(None, AXES), P(None, ("z", "y")), P(None, ("x", "core")), P(None, ("x", "core")),
        ),
        out_specs=(P(None, ("x", "core")), P(("z", "y"), ("x", "core")), P()),
        check_vma=False,
    )
```
